32 devices in a mesh: ctx: 8 (over z, y), mp: 4 (over x, core).
Axes of the slice: x: 2, y: 2, z: 4, core: 2. Of those that a mesh axis runs over, the one named last changes fastest.
Arguments:
- queries: bfloat16 [2048, 4096], P('ctx', 'mp'), may hold values from -20 to 20
- keys: bfloat16 [2048, 2048], P('ctx', 'mp'), may hold values from -20 to 20
- values: bfloat16 [2048, 2048], P('ctx', 'mp'), may hold values from -6 to 6
- out_grad: bfloat16 [2048, 4608], P('ctx', 'mp'), may hold values from -6 to 6
- doc_ids: int32 [2048], P('ctx'), may hold values from 0 to 7, never falling along the last dimension, each value on 1 to 768 neighbouring positions
- w_out: bfloat16 [4096, 4608], P('mp'), may hold values from -0.09375 to 0.09375
Outputs:
- query_gradient: bfloat16 [2048, 4096], P('ctx', 'mp')
- key_gradient: bfloat16 [2048, 2048], P('ctx', 'mp')
- value_gradient: bfloat16 [2048, 2048], P('ctx', 'mp')
The draws below stay inside these ranges and needn't reach their ends.
Inputs may be any that keep to these rules, and one draw needn't show every extreme that they name: `doc_ids`: document numbers never fall along the sequence; every document has at most (3) * 256 tokens, and some document has exactly that many.
All inputs are finite; a program needn't handle non-finite values.
Results may differ from the reference program's by a relative error of at most 0.0069.
Values may be sent and summed in bfloat16 or wider, within the bound.
No kernel may reach another device: no remote copies, remote signals or barrier semaphores. Data moves between devices by JAX's collectives and lax.ppermute only.
A program may use at most 64 MiB of HBM per device.

```python
import math
import jax
import jax.numpy as jnp
import numpy as np
from jax import lax

D = 4608
QUERY_HEADS = 32
KEY_VALUE_HEADS = 16
HEAD_SIZE = 128
SHARD_TOKENS = 256
SPAN = 4
PACKED_TOKENS = 2048
N_CTX = 8


def shared_parts(key):
    joint_factor = jax.random.fold_in(key, 7100)
    selected_rows = jax.random.randint(jax.random.fold_in(joint_factor, 1), (PACKED_TOKENS, KEY_VALUE_HEADS), 0, 32) == 0
    travel_sense = jax.random.normal(jax.random.fold_in(joint_factor, 2), (KEY_VALUE_HEADS, HEAD_SIZE), jnp.float32)
    travel_sense = travel_sense / jnp.sqrt(jnp.sum(travel_sense * travel_sense, axis=1, keepdims=True))
    return (selected_rows, travel_sense)


def seed_jitter(key, shape):
    return jnp.clip(jax.random.normal(key, shape, jnp.float32), -6.0, 6.0)


def magnitude(key, shape):
    return jnp.exp(jax.random.uniform(key, shape, jnp.float32, jnp.log(17.3), jnp.log(30.0)))


def draw_queries(key, part):
    query_groups = QUERY_HEADS // KEY_VALUE_HEADS
    selected_rows, travel_sense = shared_parts(key)
    local_portion = jax.random.fold_in(key, 7201)
    jitter = seed_jitter(jax.random.fold_in(local_portion, 1), (PACKED_TOKENS, KEY_VALUE_HEADS, query_groups, HEAD_SIZE))
    multiplier = magnitude(jax.random.fold_in(local_portion, 2), (PACKED_TOKENS, KEY_VALUE_HEADS, query_groups))
    multiplier = jnp.where(selected_rows[:, :, None], multiplier, 0.0)
    final_output = jitter + multiplier[..., None] * travel_sense[None, :, None, :]
    return jnp.clip(final_output, -20.0, 20.0).reshape(PACKED_TOKENS, QUERY_HEADS * HEAD_SIZE).astype(jnp.bfloat16)


def draw_keys(key, part):
    selected_rows, travel_sense = shared_parts(key)
    local_portion = jax.random.fold_in(key, 7302)
    jitter = seed_jitter(jax.random.fold_in(local_portion, 1), (PACKED_TOKENS, KEY_VALUE_HEADS, HEAD_SIZE))
    multiplier = magnitude(jax.random.fold_in(local_portion, 2), (PACKED_TOKENS, KEY_VALUE_HEADS))
    multiplier = jnp.where(selected_rows, multiplier, 0.0)
    final_output = jitter + multiplier[..., None] * travel_sense[None, :, :]
    return jnp.clip(final_output, -20.0, 20.0).reshape(PACKED_TOKENS, KEY_VALUE_HEADS * HEAD_SIZE).astype(jnp.bfloat16)


def block_levels(stream_key, extent, split, least, largest):
    def one(dim, blocks):
        heights = jax.random.uniform(jax.random.fold_in(jax.random.fold_in(stream_key, 6), dim), (blocks,), jnp.float32, least / len(split), largest / len(split))
        return jnp.repeat(jnp.exp(heights), extent[dim] // blocks).reshape((-1,) + (1,) * (len(extent) - dim - 1))

    loudness = one(*split[0])
    for cut in split[1:]:
        loudness = loudness * one(*cut)
    return loudness


def profile(amount, total, reach, slope):
    loads = [(1 << 20) // math.isqrt(rank ** slope) + 1 for rank in range(2, amount + 1)]
    spare, given = total - reach - (amount - 1), [1] * (amount - 1)
    while spare > 0:
        candidates = [i for i in range(amount - 1) if given[i] < reach]
        pool, remaining = sum([loads[i] for i in candidates]), spare
        for i in candidates:
            addition = min(reach - given[i], max(1, remaining * loads[i] // pool), spare)
            given[i] = given[i] + addition
            spare = spare - addition
    return np.array([reach] + given)


def uneven_parts(own_key, amount, total, bound, lean):
    if amount == 2:
        one = jax.random.randint(own_key, (), max(1, total - bound), min(bound, total - 1) + 1)
        return jnp.stack([one, total - one])
    tallies = jnp.asarray(profile(amount, total, bound, lean), jnp.int32)
    pairs = (amount - 1) // 2
    source_of, sink = tallies[1:1 + 2 * pairs:2], tallies[2:2 + 2 * pairs:2]
    room = jnp.minimum(source_of - 1, bound - sink)
    shifted = jax.random.randint(jax.random.fold_in(own_key, 1), (pairs,), 0, 1 << 20) % (room + 1)
    tallies = tallies.at[1:1 + 2 * pairs:2].set(source_of - shifted).at[2:2 + 2 * pairs:2].set(sink + shifted)
    return tallies[jax.random.permutation(jax.random.fold_in(own_key, 2), amount)]


def gaussian(key, extent, scale, limit, cuts=(), kind=jnp.bfloat16):
    loudness = block_levels(key, extent, cuts, -0.22, 0.18) if cuts else 1.0
    entries = jax.random.normal(key, extent, jnp.float32) * scale * loudness
    return jnp.minimum(jnp.maximum(entries, -limit), limit).astype(kind)


def setup_inputs(seed: int = 0) -> dict:
    key_of = jax.random.split(jax.random.key(seed), 7)
    queries = draw_queries(jax.random.fold_in(key_of[6], 71), 0)
    keys = draw_keys(jax.random.fold_in(key_of[6], 71), 0)
    values = gaussian(key_of[2], (PACKED_TOKENS, KEY_VALUE_HEADS * HEAD_SIZE), 1.0, 6.0, ((0, 8), (1, 4)))
    out_grad = gaussian(key_of[3], (PACKED_TOKENS, D), 1.0, 6.0, ((0, 8), (1, 4)))
    doc_ids = jnp.searchsorted(jnp.cumsum(uneven_parts(key_of[4], N_CTX, PACKED_TOKENS, (SPAN - 1) * SHARD_TOKENS, 2)), jnp.arange(PACKED_TOKENS), side="right").astype(jnp.int32)
    w_out = gaussian(key_of[5], (QUERY_HEADS * HEAD_SIZE, D), D ** -0.5, 0.09375, ((0, 4),))
    return {"queries": queries, "keys": keys, "values": values, "out_grad": out_grad, "doc_ids": doc_ids, "w_out": w_out}


cap_value = 50.0
query_scale = 1.0 / 12.0


def tile_scores(query_quad, key_slab):
    raw = jnp.einsum("qhgd,khd->hgqk", query_quad.astype(jnp.float32), key_slab.astype(jnp.float32))
    tanh_part = jnp.tanh(raw * (query_scale / cap_value))
    return cap_value * tanh_part, tanh_part


def reference(queries, keys, values, out_grad, doc_ids, w_out):
    query_groups = QUERY_HEADS // KEY_VALUE_HEADS
    visible_span = SPAN * SHARD_TOKENS
    leading_edge = (SPAN - 1) * SHARD_TOKENS
    padded_keys = jnp.concatenate([jnp.zeros((leading_edge, KEY_VALUE_HEADS * HEAD_SIZE), jnp.bfloat16), keys])
    padded_values = jnp.concatenate([jnp.zeros((leading_edge, KEY_VALUE_HEADS * HEAD_SIZE), jnp.bfloat16), values])
    ids_front = jnp.concatenate([jnp.full((leading_edge,), -1, jnp.int32), doc_ids])
    offsets = jnp.arange(SHARD_TOKENS, dtype=jnp.int32)
    spots = jnp.arange(visible_span, dtype=jnp.int32)
    weight_full = w_out.astype(jnp.float32)

    def query_block(index):
        span_opening = (index * SHARD_TOKENS).astype(jnp.int32)
        query_quad = lax.dynamic_slice_in_dim(queries, span_opening, SHARD_TOKENS, 0).reshape(SHARD_TOKENS, KEY_VALUE_HEADS, query_groups, HEAD_SIZE)
        grad_rows = lax.dynamic_slice_in_dim(out_grad, span_opening, SHARD_TOKENS, 0).astype(jnp.float32)
        incoming_gradient = lax.dot_general(grad_rows, weight_full, (((1,), (1,)), ((), ()))).astype(jnp.bfloat16)
        gradient_quad = incoming_gradient.reshape(SHARD_TOKENS, KEY_VALUE_HEADS, query_groups, HEAD_SIZE)
        key_slab = lax.dynamic_slice_in_dim(padded_keys, span_opening, visible_span, 0).reshape(visible_span, KEY_VALUE_HEADS, HEAD_SIZE)
        value_slab = lax.dynamic_slice_in_dim(padded_values, span_opening, visible_span, 0).reshape(visible_span, KEY_VALUE_HEADS, HEAD_SIZE)
        key_ids = lax.dynamic_slice_in_dim(ids_front, span_opening, visible_span, 0)
        query_ids = lax.dynamic_slice_in_dim(doc_ids, span_opening, SHARD_TOKENS, 0)
        key_pos = span_opening - leading_edge + spots
        query_pos = span_opening + offsets
        mask = (query_ids[:, None] == key_ids[None, :]) & (key_pos[None, :] <= query_pos[:, None])
        scores, tanh_part = tile_scores(query_quad, key_slab)
        weights = jnp.where(mask, jnp.exp(scores), 0.0)
        total = jnp.sum(weights, axis=3)
        logsum_total = jnp.log(total)
        value_sum = jnp.einsum("hgqk,khd->qhgd", weights.astype(jnp.bfloat16).astype(jnp.float32), value_slab.astype(jnp.float32))
        attended = value_sum / jnp.transpose(total, (2, 0, 1))[..., None]
        row_correction = jnp.transpose(jnp.sum(gradient_quad.astype(jnp.float32) * attended, axis=3), (1, 2, 0))
        probs = jnp.where(mask, jnp.exp(scores - logsum_total[..., None]), 0.0)
        prob_grad = jnp.einsum("qhgd,khd->hgqk", gradient_quad.astype(jnp.float32), value_slab.astype(jnp.float32))
        logit_grad = (probs * (prob_grad - row_correction[..., None]) * (1.0 - tanh_part * tanh_part) * query_scale).astype(jnp.bfloat16)
        query_part = jnp.einsum("hgqk,khd->qhgd", logit_grad.astype(jnp.float32), key_slab.astype(jnp.float32))
        return (query_part.reshape(SHARD_TOKENS, QUERY_HEADS * HEAD_SIZE).astype(jnp.bfloat16), incoming_gradient,
                jnp.transpose(logsum_total, (2, 0, 1)), jnp.transpose(row_correction, (2, 0, 1)))

    query_gradient, incoming_gradient, logsum_total, row_correction = lax.map(query_block, jnp.arange(N_CTX, dtype=jnp.int32))
    query_gradient = query_gradient.reshape(PACKED_TOKENS, QUERY_HEADS * HEAD_SIZE)
    padded_gradient = jnp.concatenate([incoming_gradient.reshape(PACKED_TOKENS, QUERY_HEADS * HEAD_SIZE), jnp.zeros((leading_edge, QUERY_HEADS * HEAD_SIZE), jnp.bfloat16)])
    padded_queries = jnp.concatenate([queries, jnp.zeros((leading_edge, QUERY_HEADS * HEAD_SIZE), jnp.bfloat16)])
    ids_back = jnp.concatenate([doc_ids, jnp.full((leading_edge,), -1, jnp.int32)])
    padded_logsum = jnp.concatenate([logsum_total.reshape(PACKED_TOKENS, KEY_VALUE_HEADS, query_groups), jnp.zeros((leading_edge, KEY_VALUE_HEADS, query_groups), jnp.float32)])
    padded_correction = jnp.concatenate([row_correction.reshape(PACKED_TOKENS, KEY_VALUE_HEADS, query_groups), jnp.zeros((leading_edge, KEY_VALUE_HEADS, query_groups), jnp.float32)])

    def key_block_grads(index):
        span_opening = (index * SHARD_TOKENS).astype(jnp.int32)
        key_slab = lax.dynamic_slice_in_dim(keys, span_opening, SHARD_TOKENS, 0).reshape(SHARD_TOKENS, KEY_VALUE_HEADS, HEAD_SIZE)
        value_slab = lax.dynamic_slice_in_dim(values, span_opening, SHARD_TOKENS, 0).reshape(SHARD_TOKENS, KEY_VALUE_HEADS, HEAD_SIZE)
        key_ids = lax.dynamic_slice_in_dim(doc_ids, span_opening, SHARD_TOKENS, 0)
        query_quad = lax.dynamic_slice_in_dim(padded_queries, span_opening, visible_span, 0).reshape(visible_span, KEY_VALUE_HEADS, query_groups, HEAD_SIZE)
        gradient_quad = lax.dynamic_slice_in_dim(padded_gradient, span_opening, visible_span, 0).reshape(visible_span, KEY_VALUE_HEADS, query_groups, HEAD_SIZE)
        query_ids = lax.dynamic_slice_in_dim(ids_back, span_opening, visible_span, 0)
        log_rows = jnp.transpose(lax.dynamic_slice_in_dim(padded_logsum, span_opening, visible_span, 0), (1, 2, 0))
        delta_rows = jnp.transpose(lax.dynamic_slice_in_dim(padded_correction, span_opening, visible_span, 0), (1, 2, 0))
        key_pos = span_opening + offsets
        query_pos = span_opening + spots
        mask = (query_ids[:, None] == key_ids[None, :]) & (key_pos[None, :] <= query_pos[:, None])
        scores, tanh_part = tile_scores(query_quad, key_slab)
        probs = jnp.where(mask, jnp.exp(scores - log_rows[..., None]), 0.0)
        prob_grad = jnp.einsum("qhgd,khd->hgqk", gradient_quad.astype(jnp.float32), value_slab.astype(jnp.float32))
        logit_grad = (probs * (prob_grad - delta_rows[..., None]) * (1.0 - tanh_part * tanh_part) * query_scale).astype(jnp.bfloat16)
        key_portion = jnp.einsum("hgqk,qhgd->khd", logit_grad.astype(jnp.float32), query_quad.astype(jnp.float32))
        value_portion = jnp.einsum("hgqk,qhgd->khd", probs.astype(jnp.bfloat16).astype(jnp.float32), gradient_quad.astype(jnp.float32))
        return (key_portion.reshape(SHARD_TOKENS, KEY_VALUE_HEADS * HEAD_SIZE).astype(jnp.bfloat16),
                value_portion.reshape(SHARD_TOKENS, KEY_VALUE_HEADS * HEAD_SIZE).astype(jnp.bfloat16))

    key_gradient, value_gradient = lax.map(key_block_grads, jnp.arange(N_CTX, dtype=jnp.int32))
    return query_gradient, key_gradient.reshape(PACKED_TOKENS, KEY_VALUE_HEADS * HEAD_SIZE), value_gradient.reshape(PACKED_TOKENS, KEY_VALUE_HEADS * HEAD_SIZE)
```

```python
import functools

import jax
import jax.numpy as jnp
from jax import lax
from jax.experimental import pallas as pl
from jax.experimental.pallas import tpu as pltpu
from jax.sharding import PartitionSpec as P

QUERY_HEADS = 32
KEY_VALUE_HEADS = 16
HEAD_SIZE = 128
SPAN = 4
GROUPS = QUERY_HEADS // KEY_VALUE_HEADS
EXTRA = 16

cap_value = 50.0
query_scale = 1.0 / 12.0


f32 = jnp.float32
bf16 = jnp.bfloat16


def passed_along(value, axis, steps):
    count = lax.axis_size(axis)
    first, last = (max(0, -steps), min(count, count - steps))
    return lax.ppermute(value, axis, [(source, source + steps) for source in range(first, last)])


def swapped(value, axis, bit):
    count = lax.axis_size(axis)
    return lax.ppermute(value, axis, [(source, source ^ bit) for source in range(count)])


def nt(a, b):
    return lax.dot_general(a, b, (((1,), (1,)), ((), ())), preferred_element_type=f32)


def nn(a, b):
    return lax.dot_general(a, b, (((1,), (0,)), ((), ())), preferred_element_type=f32)


def tn(a, b):
    return lax.dot_general(a, b, (((0,), (0,)), ((), ())), preferred_element_type=f32)


def tile_mask(qid_ref, kv_ref, rows, causal):
    chunks = rows // HEAD_SIZE
    key_ids = jnp.concatenate(
        [kv_ref[0, rows + c : rows + c + 1, :].astype(f32) for c in range(chunks)], axis=1
    )
    mask = qid_ref[:, 0:1] == key_ids
    if causal:
        row = lax.broadcasted_iota(jnp.int32, (rows, rows), 0)
        col = lax.broadcasted_iota(jnp.int32, (rows, rows), 1)
        mask = mask & (col <= row)
    return mask


def head_cols(g):
    return slice(g * HEAD_SIZE, (g + 1) * HEAD_SIZE)


def spread(column):
    return jnp.broadcast_to(column, (column.shape[0], HEAD_SIZE))


def forward_kernel(hops, fresh, rows, *refs):
    q_ref, qid_ref = refs[:2]
    kv_refs = refs[2 : 2 + len(hops)]
    rest = refs[2 + len(hops) :]
    if fresh:
        av_out, tot_out = rest
    else:
        av_in, tot_in, av_out, tot_out = rest
    masks = [tile_mask(qid_ref, kv, rows, hop == 0) for hop, kv in zip(hops, kv_refs)]
    for g in range(GROUPS):
        cols = head_cols(g)
        q = q_ref[:, cols]
        av = None if fresh else av_in[:, cols]
        tot = None if fresh else tot_in[:, cols]
        for mask, kv in zip(masks, kv_refs):
            t = jnp.tanh(nt(q, kv[0, :rows, :]) * (query_scale / cap_value))
            w = jnp.where(mask, jnp.exp(cap_value * t), 0.0)
            part = spread(jnp.sum(w, axis=1, keepdims=True))
            portion = nn(w.astype(bf16), kv[1, :rows, :])
            av = portion if av is None else av + portion
            tot = part if tot is None else tot + part
        av_out[:, cols] = av
        tot_out[:, cols] = tot


def turn_kernel(rows, q_ref, qid_ref, hg_ref, av_ref, tot_ref, kv, dq_out, inv_out, delta_out, dkv_out):
    mask = tile_mask(qid_ref, kv, rows, False)
    k = kv[0, :rows, :]
    v = kv[1, :rows, :]
    dk = dv = None
    for g in range(GROUPS):
        cols = head_cols(g)
        q = q_ref[:, cols]
        hg = hg_ref[:, cols]
        t = jnp.tanh(nt(q, k) * (query_scale / cap_value))
        w = jnp.where(mask, jnp.exp(cap_value * t), 0.0)
        tot = tot_ref[:, cols][:, 0:1] + jnp.sum(w, axis=1, keepdims=True)
        av = av_ref[:, cols] + nn(w.astype(bf16), v)
        inv = 1.0 / tot
        delta = jnp.sum(hg.astype(f32) * av, axis=1, keepdims=True) * inv
        inv_out[:, cols] = spread(inv)
        delta_out[:, cols] = spread(delta)
        p = w * inv
        lg = (p * (nt(hg, v) - delta) * ((1.0 - t * t) * query_scale)).astype(bf16)
        dq_out[:, cols] = nn(lg, k)
        dk_g = tn(lg, q)
        dv_g = tn(p.astype(bf16), hg)
        dk = dk_g if dk is None else dk + dk_g
        dv = dv_g if dv is None else dv + dv_g
    dkv_out[0] = dk.astype(dkv_out.dtype)
    dkv_out[1] = dv.astype(dkv_out.dtype)


def backward_kernel(
    causal, rows, q_ref, qid_ref, hg_ref, inv_ref, delta_ref, kv, dq_in, dq_out, dkv_out
):
    mask = tile_mask(qid_ref, kv, rows, causal)
    k = kv[0, :rows, :]
    v = kv[1, :rows, :]
    dk = dv = None
    for g in range(GROUPS):
        cols = head_cols(g)
        q = q_ref[:, cols]
        hg = hg_ref[:, cols]
        t = jnp.tanh(nt(q, k) * (query_scale / cap_value))
        p = jnp.where(mask, jnp.exp(cap_value * t), 0.0) * inv_ref[:, cols][:, 0:1]
        delta = delta_ref[:, cols][:, 0:1]
        lg = (p * (nt(hg, v) - delta) * ((1.0 - t * t) * query_scale)).astype(bf16)
        dq_out[:, cols] = (dq_in[:, cols] + nn(lg, k)).astype(dq_out.dtype)
        dk_g = tn(lg, q)
        dv_g = tn(p.astype(bf16), hg)
        dk = dk_g if dk is None else dk + dk_g
        dv = dv_g if dv is None else dv + dv_g
    dkv_out[0] = dk.astype(dkv_out.dtype)
    dkv_out[1] = dv.astype(dkv_out.dtype)


def head_grad_kernel(count, order_ref, *refs):
    pieces = refs[:count]
    w_ref, out_ref, acc = refs[count:]
    step = pl.program_id(0)
    for c in range(count):

        @pl.when(step == c)
        def _(c=c):
            part = nt(pieces[c][...], w_ref[...])
            if c == 0:
                acc[...] = part
            elif c < count - 1:
                acc[...] += part
            else:
                out_ref[...] = (acc[...] + part).astype(bf16)


def head_gradient(out_grad, w_out):
    count = lax.axis_size("mp")
    rows, chunk = out_grad.shape
    if chunk % HEAD_SIZE or count & (count - 1) or count < 2:
        full = lax.all_gather(out_grad, "mp", axis=1, tiled=True)
        return nt(full, w_out).astype(bf16)
    pieces = {0: out_grad}
    bit = count // 2
    while bit:
        pieces.update({m ^ bit: swapped(p, "mp", bit) for m, p in list(pieces.items())})
        bit //= 2
    mine = lax.axis_index("mp")
    order = (mine ^ jnp.arange(count, dtype=jnp.int32)).astype(jnp.int32)
    width = w_out.shape[0]
    return pl.pallas_call(
        functools.partial(head_grad_kernel, count),
        out_shape=jax.ShapeDtypeStruct((rows, width), bf16),
        grid_spec=pltpu.PrefetchScalarGridSpec(
            num_scalar_prefetch=1,
            grid=(count,),
            in_specs=[pl.BlockSpec((rows, chunk), lambda c, o: (0, 0))] * count
            + [pl.BlockSpec((width, chunk), lambda c, o: (0, o[c]))],
            out_specs=pl.BlockSpec((rows, width), lambda c, o: (0, 0)),
            scratch_shapes=[pltpu.VMEM((rows, width), f32)],
        ),
        cost_estimate=pl.CostEstimate(
            flops=2 * rows * width * chunk * count, transcendentals=0,
            bytes_accessed=2 * width * chunk * count,
        ),
        name="head_grad",
    )(order, *[pieces[m] for m in range(count)], w_out)


def body(queries, keys, values, out_grad, doc_ids, w_out):
    rows, width = queries.shape
    kv_width = keys.shape[1]
    kv_heads = kv_width // HEAD_SIZE
    chunks = rows // HEAD_SIZE
    ids = doc_ids.astype(f32) + 1.0
    id_rows = jnp.pad(ids.reshape(chunks, HEAD_SIZE), ((0, EXTRA - chunks), (0, 0))).astype(bf16)
    id_rows = jnp.broadcast_to(jnp.tile(id_rows, (1, kv_heads))[None], (2, EXTRA, kv_width))
    own = jnp.concatenate([jnp.stack([keys, values]), id_rows], axis=1)
    qid = jnp.broadcast_to(ids[:, None], (rows, HEAD_SIZE))

    hop1 = passed_along(own, "ctx", 1)
    hop2 = passed_along(own, "ctx", 2)
    hop3 = passed_along(hop1, "ctx", 2)
    head_grad = head_gradient(out_grad, w_out)

    wide = pl.BlockSpec((rows, GROUPS * HEAD_SIZE), lambda h: (0, h))
    whole = pl.BlockSpec((rows, HEAD_SIZE), lambda h: (0, 0))
    kv_in = pl.BlockSpec((2, rows + EXTRA, HEAD_SIZE), lambda h: (0, 0, h))
    kv_out = pl.BlockSpec((2, rows, HEAD_SIZE), lambda h: (0, 0, h))
    wide_f32 = jax.ShapeDtypeStruct((rows, width), f32)
    tile_flops = 2 * rows * rows * width

    def cost(n):
        return pl.CostEstimate(
            flops=n * tile_flops, transcendentals=0, bytes_accessed=4 * rows * width
        )

    def forward(hops, payloads, state):
        return pl.pallas_call(
            functools.partial(forward_kernel, hops, state is None, rows),
            grid=(kv_heads,),
            in_specs=[wide, whole] + [kv_in] * len(hops) + [wide] * (0 if state is None else 2),
            out_specs=[wide, wide],
            out_shape=[wide_f32, wide_f32],
            cost_estimate=cost(4 * len(hops)),
            name="forward" + "".join(map(str, hops)),
        )(queries, qid, *payloads, *(state or ()))

    def backward(hop, payload, dq, stats, final):
        return pl.pallas_call(
            functools.partial(backward_kernel, hop == 0, rows),
            grid=(kv_heads,),
            in_specs=[wide, whole, wide, wide, wide, kv_in, wide],
            out_specs=[wide, kv_out],
            out_shape=[
                jax.ShapeDtypeStruct((rows, width), bf16 if final else f32),
                jax.ShapeDtypeStruct((2, rows, kv_width), f32 if hop in (0, 1) else bf16),
            ],
            cost_estimate=cost(8),
            name="backward" + str(hop),
        )(queries, qid, head_grad, *stats, payload, dq)

    state = forward((0,), (own,), None)
    state = forward((1, 2), (hop1, hop2), state)
    dq, inv, delta, grad3 = pl.pallas_call(
        functools.partial(turn_kernel, rows),
        grid=(kv_heads,),
        in_specs=[wide, whole, wide, wide, wide, kv_in],
        out_specs=[wide, wide, wide, kv_out],
        out_shape=[
            wide_f32,
            wide_f32,
            wide_f32,
            jax.ShapeDtypeStruct((2, rows, kv_width), bf16),
        ],
        cost_estimate=cost(8),
        name="turn",
    )(queries, qid, head_grad, *state, hop3)
    stats = (inv, delta)
    back3 = passed_along(grad3, "ctx", -2)
    dq, grad2 = backward(2, hop2, dq, stats, False)
    back2 = passed_along(grad2, "ctx", -2)
    dq, grad1 = backward(1, hop1, dq, stats, False)
    back1 = passed_along((grad1 + back3.astype(f32)).astype(bf16), "ctx", -1)
    dq, grad0 = backward(0, own, dq, stats, True)
    total = grad0 + back2.astype(f32) + back1.astype(f32)
    return (dq, total[0].astype(bf16), total[1].astype(bf16))


def solution(mesh):
    placed = (
        P("ctx", "mp"),
        P("ctx", "mp"),
        P("ctx", "mp"),
        P("ctx", "mp"),
        P("ctx"),
        P("mp", None),
    )
    return jax.shard_map(
        body,
        mesh=mesh,
        in_specs=placed,
        out_specs=(P("ctx", "mp"), P("ctx", "mp"), P("ctx", "mp")),
        check_vma=False,
    )
```

```python
import functools

import jax
import jax.numpy as jnp
from jax import lax
from jax.experimental import pallas as pl
from jax.experimental.pallas import tpu as pltpu
from jax.sharding import PartitionSpec as P

QUERY_HEADS = 32
KEY_VALUE_HEADS = 16
HEAD_SIZE = 128
SPAN = 4
GROUPS = QUERY_HEADS // KEY_VALUE_HEADS
EXTRA = 16

cap_value = 50.0
query_scale = 1.0 / 12.0


f32 = jnp.float32
bf16 = jnp.bfloat16


def passed_along(value, axis, steps):
    count = lax.axis_size(axis)
    first, last = (max(0, -steps), min(count, count - steps))
    return lax.ppermute(value, axis, [(source, source + steps) for source in range(first, last)])


def swapped(value, axis, bit):
    count = lax.axis_size(axis)
    return lax.ppermute(value, axis, [(source, source ^ bit) for source in range(count)])


def nt(a, b):
    return lax.dot_general(a, b, (((1,), (1,)), ((), ())), preferred_element_type=f32)


def nn(a, b):
    return lax.dot_general(a, b, (((1,), (0,)), ((), ())), preferred_element_type=f32)


def tn(a, b):
    return lax.dot_general(a, b, (((0,), (0,)), ((), ())), preferred_element_type=f32)


def key_mask(qid_ref, kv_ref, rows, causal):
    parts = []
    for c in range(rows // HEAD_SIZE):
        row = kv_ref[0, rows + c : rows + c + 1, :].astype(f32)
        column = jnp.transpose(jnp.broadcast_to(row, (HEAD_SIZE, HEAD_SIZE)))
        parts.append(jnp.concatenate([column] * (rows // HEAD_SIZE), axis=1))
    mask = jnp.concatenate(parts, axis=0) == qid_ref[...]
    if causal:
        key = lax.broadcasted_iota(jnp.int32, (rows, rows), 0)
        query = lax.broadcasted_iota(jnp.int32, (rows, rows), 1)
        mask = mask & (key <= query)
    return mask


def head_cols(g):
    return slice(g * HEAD_SIZE, (g + 1) * HEAD_SIZE)


def weights_of(q, k, mask):
    t = jnp.tanh(nt(k, q) * (query_scale / cap_value))
    return t, jnp.where(mask, jnp.exp(cap_value * t), 0.0)


def row_sum(x):
    return jnp.sum(x, axis=0, keepdims=True)


def gradients(t, p, pg, delta, q, hg, k):
    lg = (p * (pg - delta) * ((1.0 - t * t) * query_scale)).astype(bf16)
    return tn(lg, k), nn(lg, q), nn(p.astype(bf16), hg)


def stats_kernel(hops, rows, q_ref, qid_ref, hg_ref, *refs):
    kv_refs, out = refs[:-1], refs[-1]
    masks = [key_mask(qid_ref, kv, rows, hop == 0) for hop, kv in zip(hops, kv_refs)]
    for g in range(GROUPS):
        q = q_ref[:, head_cols(g)]
        hg = hg_ref[:, head_cols(g)]
        total = delta = 0.0
        for mask, kv in zip(masks, kv_refs):
            _, w = weights_of(q, kv[0, :rows, :], mask)
            total = total + row_sum(w)
            delta = delta + row_sum(w * nt(kv[1, :rows, :], hg))
        out[0, g : g + 1, :] = total
        out[0, GROUPS + g : GROUPS + g + 1, :] = delta


def turn_kernel(rows, q_ref, qid_ref, hg_ref, sums, kv, dq_out, stats_out, dkv_out):
    mask = key_mask(qid_ref, kv, rows, False)
    k = kv[0, :rows, :]
    v = kv[1, :rows, :]
    dk = dv = 0.0
    for g in range(GROUPS):
        cols = head_cols(g)
        q = q_ref[:, cols]
        hg = hg_ref[:, cols]
        t, w = weights_of(q, k, mask)
        pg = nt(v, hg)
        inv = 1.0 / (sums[0, g : g + 1, :] + row_sum(w))
        delta = (sums[0, GROUPS + g : GROUPS + g + 1, :] + row_sum(w * pg)) * inv
        stats_out[0, g : g + 1, :] = inv
        stats_out[0, GROUPS + g : GROUPS + g + 1, :] = delta
        dq, dk_g, dv_g = gradients(t, w * inv, pg, delta, q, hg, k)
        dq_out[:, cols] = dq
        dk = dk + dk_g
        dv = dv + dv_g
    dkv_out[0] = dk.astype(dkv_out.dtype)
    dkv_out[1] = dv.astype(dkv_out.dtype)


def backward_kernel(hops, rows, q_ref, qid_ref, hg_ref, stats, *refs):
    count = len(hops)
    kv_refs, dq_in, dq_out, dkv_outs = refs[:count], refs[count], refs[count + 1], refs[count + 2 :]
    masks = [key_mask(qid_ref, kv, rows, hop == 0) for hop, kv in zip(hops, kv_refs)]
    dks = [0.0] * count
    dvs = [0.0] * count
    for g in range(GROUPS):
        cols = head_cols(g)
        q = q_ref[:, cols]
        hg = hg_ref[:, cols]
        inv = stats[0, g : g + 1, :]
        delta = stats[0, GROUPS + g : GROUPS + g + 1, :]
        dq = dq_in[:, cols]
        for n, (mask, kv) in enumerate(zip(masks, kv_refs)):
            k = kv[0, :rows, :]
            t, w = weights_of(q, k, mask)
            dq_g, dk_g, dv_g = gradients(
                t, w * inv, nt(kv[1, :rows, :], hg), delta, q, hg, k
            )
            dq = dq + dq_g
            dks[n] = dks[n] + dk_g
            dvs[n] = dvs[n] + dv_g
        dq_out[:, cols] = dq.astype(dq_out.dtype)
    for out, dk, dv in zip(dkv_outs, dks, dvs):
        out[0] = dk.astype(out.dtype)
        out[1] = dv.astype(out.dtype)


def head_grad_kernel(count, fresh, order_ref, *refs):
    pieces = refs[:count]
    if fresh:
        w_ref, out_ref, acc = refs[count:]
    else:
        w_ref, before, out_ref, acc = refs[count:]
    step = pl.program_id(1)
    for c in range(count):

        @pl.when(step == c)
        def _(c=c):
            part = nt(pieces[c][...], w_ref[...])
            if c:
                part = acc[...] + part
            elif not fresh:
                part = before[...] + part
            if c < count - 1:
                acc[...] = part
            else:
                out_ref[...] = part.astype(out_ref.dtype)


def head_grad_part(pieces, order, w_out, before):
    count = len(pieces)
    rows, chunk = pieces[0].shape
    width = w_out.shape[0]
    half = width // 2
    block = pl.BlockSpec((rows, half), lambda j, c, o: (0, j))
    return pl.pallas_call(
        functools.partial(head_grad_kernel, count, before is None),
        out_shape=jax.ShapeDtypeStruct((rows, width), f32 if before is None else bf16),
        grid_spec=pltpu.PrefetchScalarGridSpec(
            num_scalar_prefetch=1,
            grid=(2, count),
            in_specs=[pl.BlockSpec((rows, chunk), lambda j, c, o: (0, 0))] * count
            + [pl.BlockSpec((half, chunk), lambda j, c, o: (j, o[c]))]
            + [block] * (before is not None),
            out_specs=block,
            scratch_shapes=[pltpu.VMEM((rows, half), f32)],
        ),
        cost_estimate=pl.CostEstimate(
            flops=2 * rows * width * chunk * count,
            transcendentals=0,
            bytes_accessed=2 * width * chunk * count,
        ),
        name="head_grad",
    )(order, *pieces, w_out, *([] if before is None else [before]))


def head_gradient(out_grad, w_out):
    count = lax.axis_size("mp")
    chunk = out_grad.shape[1]
    if chunk % HEAD_SIZE or count & (count - 1) or count < 2:
        full = lax.all_gather(out_grad, "mp", axis=1, tiled=True)
        return nt(full, w_out).astype(bf16)
    pieces = {0: out_grad}
    bit = count // 2
    while bit:
        pieces.update({m ^ bit: swapped(p, "mp", bit) for m, p in list(pieces.items())})
        bit //= 2
    mine = lax.axis_index("mp")
    order = (mine ^ jnp.arange(count, dtype=jnp.int32)).astype(jnp.int32)
    half = count // 2
    early = head_grad_part([pieces[m] for m in range(half)], order[:half], w_out, None)
    return head_grad_part([pieces[m] for m in range(half, count)], order[half:], w_out, early)


def body(queries, keys, values, out_grad, doc_ids, w_out):
    rows, width = queries.shape
    kv_width = keys.shape[1]
    kv_heads = kv_width // HEAD_SIZE
    chunks = rows // HEAD_SIZE
    ids = doc_ids.astype(f32) + 1.0
    id_rows = jnp.pad(ids.reshape(chunks, HEAD_SIZE), ((0, EXTRA - chunks), (0, 0))).astype(bf16)
    id_rows = jnp.broadcast_to(jnp.tile(id_rows, (1, kv_heads))[None], (2, EXTRA, kv_width))
    own = jnp.concatenate([jnp.stack([keys, values]), id_rows], axis=1)
    qid = ids.reshape(1, rows)

    hop1 = passed_along(own, "ctx", 1)
    hop2 = passed_along(own, "ctx", 2)
    hop3 = passed_along(hop1, "ctx", 2)
    head_grad = head_gradient(out_grad, w_out)

    wide = pl.BlockSpec((rows, GROUPS * HEAD_SIZE), lambda h: (0, h))
    whole = pl.BlockSpec((1, rows), lambda h: (0, 0))
    stat = pl.BlockSpec((1, 8, rows), lambda h: (h, 0, 0))
    kv_in = pl.BlockSpec((2, rows + EXTRA, HEAD_SIZE), lambda h: (0, 0, h))
    kv_out = pl.BlockSpec((2, rows, HEAD_SIZE), lambda h: (0, 0, h))
    wide_f32 = jax.ShapeDtypeStruct((rows, width), f32)
    stat_shape = jax.ShapeDtypeStruct((kv_heads, 8, rows), f32)
    tile_flops = 2 * rows * rows * width

    def cost(n):
        return pl.CostEstimate(
            flops=n * tile_flops, transcendentals=0, bytes_accessed=4 * rows * width
        )

    def backward(hops, payloads, dq, stats, final):
        grads = [
            jax.ShapeDtypeStruct((2, rows, kv_width), bf16 if hop == 2 else f32) for hop in hops
        ]
        return pl.pallas_call(
            functools.partial(backward_kernel, hops, rows),
            grid=(kv_heads,),
            in_specs=[wide, whole, wide, stat] + [kv_in] * len(hops) + [wide],
            out_specs=[wide] + [kv_out] * len(hops),
            out_shape=[jax.ShapeDtypeStruct((rows, width), bf16 if final else f32)] + grads,
            cost_estimate=cost(8 * len(hops)),
            name="backward" + "".join(map(str, hops)),
        )(queries, qid, head_grad, stats, *payloads, dq)

    sums = pl.pallas_call(
        functools.partial(stats_kernel, (0, 1, 2), rows),
        grid=(kv_heads,),
        in_specs=[wide, whole, wide, kv_in, kv_in, kv_in],
        out_specs=stat,
        out_shape=stat_shape,
        cost_estimate=cost(12),
        name="stats",
    )(queries, qid, head_grad, own, hop1, hop2)
    dq, stats, grad3 = pl.pallas_call(
        functools.partial(turn_kernel, rows),
        grid=(kv_heads,),
        in_specs=[wide, whole, wide, stat, kv_in],
        out_specs=[wide, stat, kv_out],
        out_shape=[wide_f32, stat_shape, jax.ShapeDtypeStruct((2, rows, kv_width), bf16)],
        cost_estimate=cost(8),
        name="turn",
    )(queries, qid, head_grad, sums, hop3)
    back3 = passed_along(grad3, "ctx", -2)
    dq, grad2, grad1 = backward((2, 1), (hop2, hop1), dq, stats, False)
    back2 = passed_along(grad2, "ctx", -2)
    back1 = passed_along((grad1 + back3.astype(f32)).astype(bf16), "ctx", -1)
    dq, grad0 = backward((0,), (own,), dq, stats, True)
    total = grad0 + back2.astype(f32) + back1.astype(f32)
    return (dq, total[0].astype(bf16), total[1].astype(bf16))


def solution(mesh):
    placed = (
        P("ctx", "mp"),
        P("ctx", "mp"),
        P("ctx", "mp"),
        P("ctx", "mp"),
        P("ctx"),
        P("mp", None),
    )
    return jax.shard_map(
        body,
        mesh=mesh,
        in_specs=placed,
        out_specs=(P("ctx", "mp"), P("ctx", "mp"), P("ctx", "mp")),
        check_vma=False,
    )
```

```python
import functools

import jax
import jax.numpy as jnp
from jax import lax
from jax.experimental import pallas as pl
from jax.experimental.pallas import tpu as pltpu
from jax.sharding import PartitionSpec as P


QUERY_HEADS = 32
KEY_VALUE_HEADS = 16
HEAD_SIZE = 128
GROUPS = QUERY_HEADS // KEY_VALUE_HEADS
EXTRA = 16
VMEM_LIMIT = 24 * 1024 * 1024

cap_value = 50.0
query_scale = 1.0 / 12.0


f32 = jnp.float32
bf16 = jnp.bfloat16


def passed_along(value, axis, steps):
    count = lax.axis_size(axis)
    first, last = (max(0, -steps), min(count, count - steps))
    return lax.ppermute(value, axis, [(source, source + steps) for source in range(first, last)])


def swapped(value, axis, bit):
    count = lax.axis_size(axis)
    return lax.ppermute(value, axis, [(source, source ^ bit) for source in range(count)])


def nt(a, b):
    return lax.dot_general(a, b, (((1,), (1,)), ((), ())), preferred_element_type=f32)


def nn(a, b):
    return lax.dot_general(a, b, (((1,), (0,)), ((), ())), preferred_element_type=f32)


def tn(a, b):
    return lax.dot_general(a, b, (((0,), (0,)), ((), ())), preferred_element_type=f32)


def key_mask(qid_ref, kv_ref, rows, causal):
    parts = []
    for c in range(rows // HEAD_SIZE):
        row = kv_ref[0, rows + c : rows + c + 1, 0:HEAD_SIZE].astype(f32)
        column = jnp.transpose(jnp.broadcast_to(row, (HEAD_SIZE, HEAD_SIZE)))
        parts.append(jnp.concatenate([column] * (rows // HEAD_SIZE), axis=1))
    mask = jnp.concatenate(parts, axis=0) == qid_ref[...]
    if causal:
        key = lax.broadcasted_iota(jnp.int32, (rows, rows), 0)
        query = lax.broadcasted_iota(jnp.int32, (rows, rows), 1)
        mask = mask & (key <= query)
    return mask


def weights_of(q, k, mask):
    t = jnp.tanh(nt(k, q) * (query_scale / cap_value))
    return t, jnp.where(mask, jnp.exp(cap_value * t), 0.0)


def row_sum(x):
    return jnp.sum(x, axis=0, keepdims=True)


def gradients(t, p, pg, delta, q, hg, k):
    lg = (p * (pg - delta) * ((1.0 - t * t) * query_scale)).astype(bf16)
    return tn(lg, k), nn(lg, q), nn(p.astype(bf16), hg)


def lanes(start, size):
    return pl.ds(pl.multiple_of(start, HEAD_SIZE), size)


def per_head(kv_heads, step):
    def run(h, carry):
        step(h)
        return carry

    lax.fori_loop(0, kv_heads, run, 0)


def rounded(w):
    return w.astype(bf16).astype(f32)


def stats_kernel(hops, rows, q_ref, qid_ref, hg_ref, *refs):
    kv_refs, out = refs[:-1], refs[-1]

    def step(h):
        masks = [key_mask(qid_ref, kv, rows, hop == 0) for hop, kv in zip(hops, kv_refs)]
        mine = lanes(h * HEAD_SIZE, HEAD_SIZE)
        for g in range(GROUPS):
            cols = lanes((h * GROUPS + g) * HEAD_SIZE, HEAD_SIZE)
            q = q_ref[:, cols]
            hg = hg_ref[:, cols]
            total = delta = 0.0
            for mask, kv in zip(masks, kv_refs):
                _, w = weights_of(q, kv[0, :rows, mine], mask)
                total = total + row_sum(w)
                delta = delta + row_sum(rounded(w) * nt(kv[1, :rows, mine], hg))
            out[h, g : g + 1, :] = total
            out[h, GROUPS + g : GROUPS + g + 1, :] = delta

    per_head(out.shape[0], step)


def turn_kernel(rows, q_ref, qid_ref, hg_ref, sums, kv, dq_out, stats_out, dkv_out):
    def step(h):
        mask = key_mask(qid_ref, kv, rows, False)
        mine = lanes(h * HEAD_SIZE, HEAD_SIZE)
        k = kv[0, :rows, mine]
        v = kv[1, :rows, mine]
        dk = dv = 0.0
        for g in range(GROUPS):
            cols = lanes((h * GROUPS + g) * HEAD_SIZE, HEAD_SIZE)
            q = q_ref[:, cols]
            hg = hg_ref[:, cols]
            t, w = weights_of(q, k, mask)
            pg = nt(v, hg)
            inv = 1.0 / (sums[h, g : g + 1, :] + row_sum(w))
            delta = (sums[h, GROUPS + g : GROUPS + g + 1, :] + row_sum(rounded(w) * pg)) * inv
            stats_out[h, g : g + 1, :] = inv
            stats_out[h, GROUPS + g : GROUPS + g + 1, :] = delta
            dq, dk_g, dv_g = gradients(t, w * inv, pg, delta, q, hg, k)
            dq_out[:, cols] = dq
            dk = dk + dk_g
            dv = dv + dv_g
        dkv_out[0, :, mine] = dk.astype(dkv_out.dtype)
        dkv_out[1, :, mine] = dv.astype(dkv_out.dtype)

    per_head(sums.shape[0], step)


def backward_kernel(hops, rows, q_ref, qid_ref, hg_ref, stats, *refs):
    count = len(hops)
    kv_refs, dq_in, dq_out, dkv_outs = refs[:count], refs[count], refs[count + 1], refs[count + 2 :]

    def step(h):
        masks = [key_mask(qid_ref, kv, rows, hop == 0) for hop, kv in zip(hops, kv_refs)]
        mine = lanes(h * HEAD_SIZE, HEAD_SIZE)
        dks = [0.0] * count
        dvs = [0.0] * count
        for g in range(GROUPS):
            cols = lanes((h * GROUPS + g) * HEAD_SIZE, HEAD_SIZE)
            q = q_ref[:, cols]
            hg = hg_ref[:, cols]
            inv = stats[h, g : g + 1, :]
            delta = stats[h, GROUPS + g : GROUPS + g + 1, :]
            dq = dq_in[:, cols]
            for n, (mask, kv) in enumerate(zip(masks, kv_refs)):
                k = kv[0, :rows, mine]
                t, w = weights_of(q, k, mask)
                dq_g, dk_g, dv_g = gradients(
                    t, w * inv, nt(kv[1, :rows, mine], hg), delta, q, hg, k
                )
                dq = dq + dq_g
                dks[n] = dks[n] + dk_g
                dvs[n] = dvs[n] + dv_g
            dq_out[:, cols] = dq.astype(dq_out.dtype)
        for out, dk, dv in zip(dkv_outs, dks, dvs):
            out[0, :, mine] = dk.astype(out.dtype)
            out[1, :, mine] = dv.astype(out.dtype)

    per_head(stats.shape[0], step)


def head_grad_kernel(count, fresh, order_ref, *refs):
    pieces = refs[:count]
    w_ref, out_ref = refs[count], refs[-1]
    chunk = pieces[0].shape[1]
    total = None if fresh else refs[count + 1][...]
    for c in range(count):
        part = nt(pieces[c][...], w_ref[:, lanes(order_ref[c] * chunk, chunk)])
        total = part if total is None else total + part
    out_ref[...] = total.astype(out_ref.dtype)


def head_grad_part(pieces, order, w_out, before):
    count = len(pieces)
    rows, chunk = pieces[0].shape
    width = w_out.shape[0]
    vmem = pl.BlockSpec(memory_space=pltpu.VMEM)
    rest = [] if before is None else [before]
    return pl.pallas_call(
        functools.partial(head_grad_kernel, count, before is None),
        out_shape=jax.ShapeDtypeStruct((rows, width), f32 if before is None else bf16),
        in_specs=[pl.BlockSpec(memory_space=pltpu.SMEM)] + [vmem] * (count + 1 + len(rest)),
        out_specs=vmem,
        cost_estimate=pl.CostEstimate(
            flops=2 * rows * width * chunk * count,
            transcendentals=0,
            bytes_accessed=2 * width * chunk * count,
        ),
        compiler_params=pltpu.CompilerParams(vmem_limit_bytes=VMEM_LIMIT),
        name="head_grad",
    )(order, *pieces, w_out, *rest)


def head_gradient(out_grad, w_out):
    count = lax.axis_size("mp")
    chunk = out_grad.shape[1]
    if chunk % HEAD_SIZE or count & (count - 1) or count < 2:
        full = lax.all_gather(out_grad, "mp", axis=1, tiled=True)
        return nt(full, w_out).astype(bf16)
    pieces = {0: out_grad}
    bit = count // 2
    while bit:
        for m, p in list(pieces.items()):
            pieces[m ^ bit] = swapped(p, "mp", bit)
        bit //= 2
    mine = lax.axis_index("mp")
    order = (mine ^ jnp.arange(count, dtype=jnp.int32)).astype(jnp.int32)
    half = count // 2
    early = head_grad_part([pieces[m] for m in range(half)], order[:half], w_out, None)
    late = [pieces[m] for m in range(half, count)]
    return head_grad_part(late, order[half:], w_out, early)


def step_body(queries, keys, values, out_grad, doc_ids, w_out):
    rows, width = queries.shape
    kv_width = keys.shape[1]
    kv_heads = kv_width // HEAD_SIZE
    chunks = rows // HEAD_SIZE
    ids = doc_ids.astype(f32) + 1.0
    id_rows = jnp.pad(ids.reshape(chunks, HEAD_SIZE), ((0, EXTRA - chunks), (0, 0))).astype(bf16)
    id_rows = jnp.broadcast_to(jnp.tile(id_rows, (1, kv_heads))[None], (2, EXTRA, kv_width))
    own = jnp.concatenate([jnp.stack([keys, values]), id_rows], axis=1)
    qid = ids.reshape(1, rows)

    hop1 = passed_along(own, "ctx", 1)
    hop2 = passed_along(own, "ctx", 2)
    hop3 = passed_along(hop1, "ctx", 2)
    head_grad = head_gradient(out_grad, w_out)

    wide = whole = stat = kv_in = kv_out = pl.BlockSpec(memory_space=pltpu.VMEM)
    wide_f32 = jax.ShapeDtypeStruct((rows, width), f32)
    stat_shape = jax.ShapeDtypeStruct((kv_heads, 8, rows), f32)
    tile_flops = 2 * rows * rows * width

    def cost(n):
        return pl.CostEstimate(
            flops=n * tile_flops, transcendentals=0, bytes_accessed=4 * rows * width
        )

    def backward(hops, payloads, dq, stats, final):
        grads = [
            jax.ShapeDtypeStruct((2, rows, kv_width), bf16 if hop == 2 else f32) for hop in hops
        ]
        return pl.pallas_call(
            functools.partial(backward_kernel, hops, rows),
            in_specs=[wide, whole, wide, stat] + [kv_in] * len(hops) + [wide],
            out_specs=[wide] + [kv_out] * len(hops),
            out_shape=[jax.ShapeDtypeStruct((rows, width), bf16 if final else f32)] + grads,
            cost_estimate=cost(8 * len(hops)),
            compiler_params=pltpu.CompilerParams(vmem_limit_bytes=VMEM_LIMIT),
        )(queries, qid, head_grad, stats, *payloads, dq)

    sums = pl.pallas_call(
        functools.partial(stats_kernel, (0, 1, 2), rows),
        in_specs=[wide, whole, wide, kv_in, kv_in, kv_in],
        out_specs=stat,
        out_shape=stat_shape,
        cost_estimate=cost(12),
        compiler_params=pltpu.CompilerParams(vmem_limit_bytes=VMEM_LIMIT),
        name="stats",
    )(queries, qid, head_grad, own, hop1, hop2)
    dq, stats, grad3 = pl.pallas_call(
        functools.partial(turn_kernel, rows),
        in_specs=[wide, whole, wide, stat, kv_in],
        out_specs=[wide, stat, kv_out],
        out_shape=[wide_f32, stat_shape, jax.ShapeDtypeStruct((2, rows, kv_width), bf16)],
        cost_estimate=cost(8),
        compiler_params=pltpu.CompilerParams(vmem_limit_bytes=VMEM_LIMIT),
        name="turn",
    )(queries, qid, head_grad, sums, hop3)
    back3 = passed_along(grad3, "ctx", -2)
    dq, grad2, grad1 = backward((2, 1), (hop2, hop1), dq, stats, False)
    back2 = passed_along(grad2, "ctx", -2)
    back1 = passed_along((grad1 + back3.astype(f32)).astype(bf16), "ctx", -1)
    dq, grad0 = backward((0,), (own,), dq, stats, True)
    total = grad0 + back2.astype(f32) + back1.astype(f32)
    return (dq, total[0].astype(bf16), total[1].astype(bf16))


def solution(mesh):
    placed = (
        P("ctx", "mp"),
        P("ctx", "mp"),
        P("ctx", "mp"),
        P("ctx", "mp"),
        P("ctx"),
        P("mp", None),
    )
    return jax.shard_map(
        step_body,
        mesh=mesh,
        in_specs=placed,
        out_specs=(P("ctx", "mp"), P("ctx", "mp"), P("ctx", "mp")),
        check_vma=False,
    )
```
